32 devices in a mesh: clip: 2 (over y), ha: 4 (over z), wa: 4 (over x, core).
Axes of the slice: x: 2, y: 2, z: 4, core: 2. Of those that a mesh axis runs over, the one named last changes fastest.
Arguments:
- cotangent: float32 [8, 16, 256, 96], P('clip', 'ha', 'wa'), parts along dimension 0, may hold values from -6 to 6
- stored_first: float32 [8, 16, 256, 96], P('clip', 'ha', 'wa'), parts along dimension 0, may hold values from -8 to 8
- stored_second: float32 [8, 16, 256, 96], P('clip', 'ha', 'wa'), parts along dimension 0, may hold values from -8 to 8
- w_first: float32 [3, 3, 3, 96, 96], replicated, may hold values from -0.125 to 0.125
- w_second: float32 [3, 3, 3, 96, 96], replicated, may hold values from -0.125 to 0.125
- w_third: float32 [3, 3, 3, 96, 96], replicated, may hold values from -0.125 to 0.125
Outputs:
- input_grad: float32 [8, 16, 256, 96], P('clip', 'ha', 'wa'), parts along dimension 0
The draws below stay inside these ranges and needn't reach their ends.
There are 2 independent parts, one for each index of `clip`. The reference program is written for one: setup_inputs(seed, part) draws one part's arguments, and reference() takes and returns one part's arrays. A program takes and returns all parts, laid end to end along the dimension named above; an argument that names none is the same for every part. Nothing has to cross between parts.
All inputs are finite; a program needn't handle non-finite values.
Results may differ from the reference program's by a relative error of at most 0.00013.
Values sent between devices are 32-bit elements; how exact they have to be, the bound alone decides.
A program may use at most 64 MiB of HBM per device.

```python
import jax
import jax.numpy as jnp
from jax import lax

C = 96
F = 4
H = 16
W = 256


def levels(stream_key, extent, shards, smallest, top_value):
    loudness, own = 1.0, jax.random.fold_in(stream_key, 6)
    for position, parts in shards:
        steps = jnp.exp(jax.random.uniform(jax.random.fold_in(own, position), (parts,), jnp.float32, smallest / len(shards), top_value / len(shards)))
        loudness = loudness * jnp.repeat(steps, extent[position] // parts).reshape([-1 if axis == position else 1 for axis in range(len(extent))])
    return loudness


def bell_draw(key, dims, scale, limit, cuts=(), kind=jnp.bfloat16):
    drawn = scale * jax.random.normal(key, dims, jnp.float32)
    if cuts:
        drawn = drawn * levels(key, dims, cuts, -0.22, 0.18)
    return jnp.clip(drawn, -limit, limit).astype(kind)


def setup_inputs(seed: int = 0, part: int = 0) -> dict:
    splits = jax.random.split(jax.random.key(seed), 7)
    own_keys = jax.random.split(jax.random.fold_in(splits[6], part), 7)
    cotangent = bell_draw(own_keys[0], (F, H, W, C), 1.0, 6.0, ((1, 4), (2, 4)), jnp.float32)
    stored_first = bell_draw(own_keys[1], (F, H, W, C), 2.0, 8.0, ((1, 4), (2, 4)), jnp.float32)
    stored_second = bell_draw(own_keys[2], (F, H, W, C), 2.0, 8.0, ((1, 4), (2, 4)), jnp.float32)
    w_first = bell_draw(splits[3], (3, 3, 3, C, C), (27 * C) ** -0.5, 0.125, (), jnp.float32)
    w_second = bell_draw(splits[4], (3, 3, 3, C, C), (27 * C) ** -0.5, 0.125, (), jnp.float32)
    w_third = bell_draw(splits[5], (3, 3, 3, C, C), (27 * C) ** -0.5, 0.125, (), jnp.float32)
    return dict(cotangent=cotangent, stored_first=stored_first, stored_second=stored_second, w_first=w_first, w_second=w_second, w_third=w_third)


def back_conv(gradient, kernel):
    padded = jnp.pad(gradient, ((0, 2), (1, 1), (1, 1), (0, 0)))
    flipped = jnp.transpose(jnp.flip(kernel, (0, 1, 2)), (0, 1, 2, 4, 3))
    result = lax.conv_general_dilated(padded[None], flipped, (1, 1, 1), "VALID",
                                      dimension_numbers=("NDHWC", "DHWIO", "NDHWC"),
                                      precision=lax.Precision.HIGHEST)
    return result[0]


def silu_slope(value):
    sigma = jax.nn.sigmoid(value)
    return sigma * (1.0 + value * (1.0 - sigma))


def reference(cotangent, stored_first, stored_second, w_first, w_second, w_third):
    second_grad = back_conv(cotangent, w_third) * silu_slope(stored_second)
    first_grad = back_conv(second_grad, w_second) * silu_slope(stored_first)
    return back_conv(first_grad, w_first)
```

```python
import functools

import jax
import jax.numpy as jnp
from jax import lax
from jax.experimental import pallas as pl
from jax.experimental.pallas import tpu as pltpu
from jax.sharding import PartitionSpec as P

LANES = 128
EDGE = 8
SIDES = tuple((dh, dw) for dh in (-1, 0, 1) for dw in (-1, 0, 1) if (dh, dw) != (0, 0))
COLS = ((0, -1), (0, 1))
ROWS = tuple(s for s in SIDES if s[0] != 0)


def silu_slope(value):
    sigma = 1.0 / (1.0 + jnp.exp(-value))
    return sigma * (1.0 + value * (1.0 - sigma))


def split(value):
    high = value.astype(jnp.bfloat16)
    low = (value - high.astype(jnp.float32)).astype(jnp.bfloat16)
    return high, low


def kernel(
    sizes, cot, first, second, w1, w2, w3, out,
    ext0, ext1, ext2, xs, wbuf0, wbuf1, wbuf2, whl, acc, sfirst, ssecond,
    local_sem, send_sem, recv_sem,
):
    nh, nw, F, R, W, C = sizes
    span = 3 * LANES
    exts = (ext0, ext1, ext2)
    wbufs = (wbuf0, wbuf1, wbuf2)
    ih, iw = lax.axis_index("ha"), lax.axis_index("wa")

    def present(dh, dw):
        ok = ih >= 0
        if dh:
            ok = ok & ((ih > 0) if dh < 0 else (ih < nh - 1))
        if dw:
            ok = ok & ((iw > 0) if dw < 0 else (iw < nw - 1))
        return ok

    def one(flag):
        return jnp.where(flag, jnp.int32(1), jnp.int32(0))

    loads = [
        pltpu.make_async_copy(cot, ext0.at[:, pl.ds(1, R), pl.ds(EDGE, W), :], local_sem.at[0]),
        pltpu.make_async_copy(w3, wbuf0, local_sem.at[1]),
        pltpu.make_async_copy(w2, wbuf1, local_sem.at[2]),
        pltpu.make_async_copy(w1, wbuf2, local_sem.at[3]),
        pltpu.make_async_copy(second, ssecond, local_sem.at[4]),
        pltpu.make_async_copy(first, sfirst, local_sem.at[5]),
    ]
    for load in loads:
        load.start()

    barrier = pltpu.get_barrier_semaphore()
    for dh, dw in SIDES:
        @pl.when(present(dh, dw))
        def _():
            pl.semaphore_signal(
                barrier, inc=1, device_id={"ha": ih + dh, "wa": iw + dw},
                device_id_type=pl.DeviceIdType.MESH,
            )
    tall = 1 + one(ih > 0) + one(ih < nh - 1)
    wide = 1 + one(iw > 0) + one(iw < nw - 1)
    pl.semaphore_wait(barrier, tall * wide - 1)

    def copy_to(phase, dh, dw):
        row, rows = {-1: (0, 1), 0: (0, R), 1: (R - 1, 1)}[dh]
        col, cols = {-1: (0, EDGE), 0: (0, W), 1: (W - EDGE, EDGE)}[dw]
        drow = {-1: R + 1, 0: 1, 1: 0}[dh]
        dcol = {-1: EDGE + W, 0: EDGE, 1: 0}[dw]
        ext = exts[phase]
        if phase == 0:
            src = cot.at[:, pl.ds(row, rows), pl.ds(col, cols), :]
        else:
            src = ext.at[:, pl.ds(row + 1, rows), pl.ds(col + EDGE, cols), :]
        at = SIDES.index((dh, dw))
        return pltpu.make_async_remote_copy(
            src_ref=src,
            dst_ref=ext.at[:, pl.ds(drow, rows), pl.ds(dcol, cols), :],
            send_sem=send_sem.at[phase, at],
            recv_sem=recv_sem.at[phase, at],
            device_id={"ha": ih + dh, "wa": iw + dw},
            device_id_type=pl.DeviceIdType.MESH,
        )

    def send(phase):
        for dh, dw in COLS + ROWS:
            @pl.when(present(dh, dw))
            def _():
                copy_to(phase, dh, dw).start()

    def receive(phase, sides):
        for dh, dw in sides:
            @pl.when(present(-dh, -dw))
            def _():
                copy_to(phase, dh, dw).wait_recv()

    send(0)

    xs[...] = jnp.zeros_like(xs)
    whl[...] = jnp.zeros_like(whl)
    for dh, dw in SIDES:
        @pl.when(jnp.logical_not(present(dh, dw)))
        def _():
            row, rows = {-1: (0, 1), 0: (1, R), 1: (R + 1, 1)}[dh]
            col, cols = {-1: (0, EDGE), 0: (EDGE, W), 1: (EDGE + W, EDGE)}[dw]
            for ext in exts:
                ext[:, row : row + rows, col : col + cols, :] = jnp.zeros(
                    (F, rows, cols, C), jnp.float32
                )

    def prepare(phase):
        wbuf = wbufs[phase]

        @pl.loop(0, 3)
        def _(i):
            for j in range(3):
                for k in range(3):
                    high, low = split(wbuf[i, j, k])
                    whl[i, j, 0:C, k * LANES : k * LANES + C] = high
                    whl[i, j, 0:C, span + k * LANES : span + k * LANES + C] = low

    def arrange(phase, rows):
        ext = exts[phase]

        @pl.loop(0, F)
        def _(f):
            for e in rows:
                for k in range(3):
                    start = EDGE + 1 - k
                    high, low = split(ext[f, e, start : start + W, :])
                    xs[f, e, :, k * LANES : k * LANES + C] = high
                    xs[f, e, :, span + k * LANES : span + k * LANES + C] = low

    pairs = R // 2

    def lhs(i, q):
        shift, frames = 2 - i, F - (2 - i)
        parts = [
            xs[shift : shift + frames, 2 * p + q][:, None] for p in range(pairs)
        ]
        block = jnp.concatenate(parts, axis=1).reshape(frames * pairs * W, 2 * span)
        return jnp.concatenate([block, block[:, :span]], axis=1)

    def rhs(i, j):
        high, low = whl[i, j, :, :span], whl[i, j, :, span:]
        return jnp.concatenate([high, high, low], axis=1)

    def dot(a, b):
        return lax.dot_general(
            a, b, (((1,), (1,)), ((), ())), preferred_element_type=jnp.float32
        )

    def inner():
        for i in (2, 1, 0):
            frames = F - (2 - i)
            a = jnp.concatenate([lhs(i, 1), lhs(i, 2)], axis=1)
            b = jnp.concatenate(
                [
                    jnp.concatenate([rhs(i, 1), rhs(i, 0)], axis=1),
                    jnp.concatenate([rhs(i, 2), rhs(i, 1)], axis=1),
                ],
                axis=0,
            )
            value = dot(a, b).reshape(frames, pairs, W, 2 * LANES)
            if i == 2:
                acc[...] = value
            else:
                acc[0:frames] += value

    def outer():
        for i in (2, 1, 0):
            frames = F - (2 - i)
            for q, j, at in ((0, 2, 0), (3, 0, LANES)):
                value = dot(lhs(i, q), rhs(i, j)).reshape(frames, pairs, W, LANES)
                acc[0:frames, :, :, at : at + LANES] += value

    def result(p, half):
        return acc[:, p, :, half * LANES : half * LANES + C]

    for phase in range(3):
        loads[phase + 1].wait()
        prepare(phase)
        if phase == 0:
            loads[0].wait()
        receive(phase, COLS)
        arrange(phase, range(1, R + 1))
        inner()
        receive(phase, ROWS)
        arrange(phase, (0, R + 1))
        outer()
        if phase < 2:
            loads[4 + phase].wait()
            stored = (ssecond, sfirst)[phase]
            for h in range(R):
                exts[phase + 1][:, h + 1, EDGE : EDGE + W, :] = result(h // 2, h % 2) * silu_slope(
                    stored[:, h]
                )
            send(phase + 1)
        else:
            for h in range(R):
                out[:, h] = result(h // 2, h % 2)

    for phase in range(3):
        for dh, dw in SIDES:
            @pl.when(present(dh, dw))
            def _():
                copy_to(phase, dh, dw).wait_send()


def local(cotangent, stored_first, stored_second, w_first, w_second, w_third):
    F, R, W, C = cotangent.shape
    sizes = (lax.axis_size("ha"), lax.axis_size("wa"), F, R, W, C)
    ext = pltpu.VMEM((F, R + 2, W + 2 * EDGE, C), jnp.float32)
    wbuf = pltpu.VMEM(w_first.shape, jnp.float32)
    stored = pltpu.VMEM((F, R, W, C), jnp.float32)
    return pl.pallas_call(
        functools.partial(kernel, sizes),
        out_shape=jax.ShapeDtypeStruct(cotangent.shape, jnp.float32),
        in_specs=[pl.BlockSpec(memory_space=pl.ANY)] * 6,
        out_specs=pl.BlockSpec(memory_space=pltpu.VMEM),
        scratch_shapes=[
            ext, ext, ext,
            pltpu.VMEM((F, R + 2, W, 6 * LANES), jnp.bfloat16),
            wbuf, wbuf, wbuf,
            pltpu.VMEM((3, 3, LANES, 6 * LANES), jnp.bfloat16),
            pltpu.VMEM((F, R // 2, W, 2 * LANES), jnp.float32),
            stored, stored,
            pltpu.SemaphoreType.DMA((6,)),
            pltpu.SemaphoreType.DMA((3, 8)),
            pltpu.SemaphoreType.DMA((3, 8)),
        ],
        compiler_params=pltpu.CompilerParams(
            collective_id=0, has_side_effects=True, vmem_limit_bytes=48 * 1024 * 1024
        ),
    )(cotangent, stored_first, stored_second, w_first, w_second, w_third)


def solution(mesh):
    split_spec = P("clip", "ha", "wa", None)
    return jax.shard_map(
        local,
        mesh=mesh,
        in_specs=(split_spec, split_spec, split_spec, P(), P(), P()),
        out_specs=split_spec,
        check_vma=False,
    )
```

```python
import functools

import jax
import jax.numpy as jnp
from jax import lax
from jax.experimental import pallas as pl
from jax.experimental.pallas import tpu as pltpu
from jax.sharding import PartitionSpec as P

LANES = 128
EDGE = 8
SIDES = tuple((dh, dw) for dh in (-1, 0, 1) for dw in (-1, 0, 1) if (dh, dw) != (0, 0))
COLS = ((0, -1), (0, 1))
ROWS = tuple(s for s in SIDES if s[0] != 0)


def silu_slope(value):
    sigma = 1.0 / (1.0 + jnp.exp(-value))
    return sigma * (1.0 + value * (1.0 - sigma))


def split(value):
    high = value.astype(jnp.bfloat16)
    low = (value - high.astype(jnp.float32)).astype(jnp.bfloat16)
    return high, low


def kernel(
    sizes, cot, first, second, w1, w2, w3, out,
    ext0, ext1, ext2, xs, wbuf0, wbuf1, wbuf2, whl, acc, sfirst, ssecond,
    local_sem, send_sem, recv_sem,
):
    nh, nw, F, R, W, C = sizes
    span = 3 * LANES
    exts = (ext0, ext1, ext2)
    wbufs = (wbuf0, wbuf1, wbuf2)
    ih, iw = lax.axis_index("ha"), lax.axis_index("wa")

    def present(dh, dw):
        ok = ih >= 0
        if dh:
            ok = ok & ((ih > 0) if dh < 0 else (ih < nh - 1))
        if dw:
            ok = ok & ((iw > 0) if dw < 0 else (iw < nw - 1))
        return ok

    def one(flag):
        return jnp.where(flag, jnp.int32(1), jnp.int32(0))

    loads = [
        pltpu.make_async_copy(cot, ext0.at[:, pl.ds(1, R), pl.ds(EDGE, W), :], local_sem.at[0]),
        pltpu.make_async_copy(w3, wbuf0, local_sem.at[1]),
        pltpu.make_async_copy(w2, wbuf1, local_sem.at[2]),
        pltpu.make_async_copy(w1, wbuf2, local_sem.at[3]),
        pltpu.make_async_copy(second, ssecond, local_sem.at[4]),
        pltpu.make_async_copy(first, sfirst, local_sem.at[5]),
    ]
    for load in loads:
        load.start()

    barrier = pltpu.get_barrier_semaphore()
    for dh, dw in SIDES:
        @pl.when(present(dh, dw))
        def _():
            pl.semaphore_signal(
                barrier, inc=1, device_id={"ha": ih + dh, "wa": iw + dw},
                device_id_type=pl.DeviceIdType.MESH,
            )
    tall = 1 + one(ih > 0) + one(ih < nh - 1)
    wide = 1 + one(iw > 0) + one(iw < nw - 1)
    pl.semaphore_wait(barrier, tall * wide - 1)

    groups = ((F // 2, F), (0, F // 2))

    def copy_to(phase, group, dh, dw):
        t0, t1 = groups[group]
        row, rows = {-1: (0, 1), 0: (0, R), 1: (R - 1, 1)}[dh]
        col, cols = {-1: (0, EDGE), 0: (0, W), 1: (W - EDGE, EDGE)}[dw]
        drow = {-1: R + 1, 0: 1, 1: 0}[dh]
        dcol = {-1: EDGE + W, 0: EDGE, 1: 0}[dw]
        ext, frames = exts[phase], pl.ds(t0, t1 - t0)
        if phase == 0:
            src = cot.at[frames, pl.ds(row, rows), pl.ds(col, cols), :]
        else:
            src = ext.at[frames, pl.ds(row + 1, rows), pl.ds(col + EDGE, cols), :]
        at = SIDES.index((dh, dw))
        return pltpu.make_async_remote_copy(
            src_ref=src,
            dst_ref=ext.at[frames, pl.ds(drow, rows), pl.ds(dcol, cols), :],
            send_sem=send_sem.at[phase, group, at],
            recv_sem=recv_sem.at[phase, group, at],
            device_id={"ha": ih + dh, "wa": iw + dw},
            device_id_type=pl.DeviceIdType.MESH,
        )

    def send(phase, group):
        for dh, dw in COLS + ROWS:
            @pl.when(present(dh, dw))
            def _():
                copy_to(phase, group, dh, dw).start()

    def receive(phase, group, sides):
        for dh, dw in sides:
            @pl.when(present(-dh, -dw))
            def _():
                copy_to(phase, group, dh, dw).wait_recv()

    send(0, 0)
    send(0, 1)

    xs[...] = jnp.zeros_like(xs)
    for dh, dw in SIDES:
        @pl.when(jnp.logical_not(present(dh, dw)))
        def _():
            row, rows = {-1: (0, 1), 0: (1, R), 1: (R + 1, 1)}[dh]
            col, cols = {-1: (0, EDGE), 0: (EDGE, W), 1: (EDGE + W, EDGE)}[dw]
            for ext in exts:
                ext[:, row : row + rows, col : col + cols, :] = jnp.zeros(
                    (F, rows, cols, C), jnp.float32
                )

    def prepare(phase):
        wbuf = wbufs[phase]

        @pl.loop(0, 3)
        def _(i):
            for j in range(3):
                for k in range(3):
                    turned = split(jnp.transpose(wbuf[i, j, k]))
                    for part in range(2):
                        at = part * span + k * LANES
                        whl[phase, i, j, at : at + C, 0:C] = turned[part]
                        whl[phase, i, j, at + C : at + LANES, :] = jnp.zeros(
                            (LANES - C, LANES), jnp.bfloat16
                        )

    def arrange(phase, group, rows):
        ext = exts[phase]

        @pl.loop(*groups[group])
        def _(f):
            for e in rows:
                for k in range(3):
                    start = EDGE + 1 - k
                    high, low = split(ext[f, e, start : start + W, :])
                    xs[f, e, :, k * LANES : k * LANES + C] = high
                    xs[f, e, :, span + k * LANES : span + k * LANES + C] = low

    pairs = R // 2

    def reach(group, i):
        t0, t1 = groups[group]
        return t0, min(t1, F - 2 + i)

    def lhs(group, i, q):
        t0, t1 = reach(group, i)
        parts = [xs[t0 + 2 - i : t1 + 2 - i, 2 * p + q][:, None] for p in range(pairs)]
        block = jnp.concatenate(parts, axis=1).reshape((t1 - t0) * pairs * W, 2 * span)
        return jnp.concatenate([block, block[:, :span]], axis=1)

    def rhs(phase, i, j):
        high, low = whl[phase, i, j, :span], whl[phase, i, j, span:]
        return jnp.concatenate([high, high, low], axis=0)

    def dot(a, b):
        return jnp.dot(a, b, preferred_element_type=jnp.float32)

    def inner(phase, group):
        for i in (2, 1, 0):
            t0, t1 = reach(group, i)
            if t1 <= t0:
                continue
            a = jnp.concatenate([lhs(group, i, 1), lhs(group, i, 2)], axis=1)
            b = jnp.concatenate(
                [
                    jnp.concatenate([rhs(phase, i, 1), rhs(phase, i, 2)], axis=1),
                    jnp.concatenate([rhs(phase, i, 0), rhs(phase, i, 1)], axis=1),
                ],
                axis=0,
            )
            value = dot(a, b).reshape(t1 - t0, pairs, W, 2 * LANES)
            if i == 2:
                acc[t0:t1] = value
            else:
                acc[t0:t1] += value

    def outer(phase, group):
        for i in (2, 1, 0):
            t0, t1 = reach(group, i)
            if t1 <= t0:
                continue
            for q, j, at in ((0, 2, 0), (3, 0, LANES)):
                value = dot(lhs(group, i, q), rhs(phase, i, j)).reshape(t1 - t0, pairs, W, LANES)
                acc[t0:t1, :, :, at : at + LANES] += value

    for phase in range(3):
        loads[phase + 1].wait()
        prepare(phase)
    loads[0].wait()
    for phase in range(3):
        for group in range(2):
            t0, t1 = groups[group]
            receive(phase, group, COLS)
            arrange(phase, group, range(1, R + 1))
            inner(phase, group)
            receive(phase, group, ROWS)
            arrange(phase, group, (0, R + 1))
            outer(phase, group)
            if phase < 2 and group == 0:
                loads[4 + phase].wait()
            for h in range(R):
                at = h % 2 * LANES
                value = acc[t0:t1, h // 2, :, at : at + C]
                if phase < 2:
                    stored = (ssecond, sfirst)[phase]
                    exts[phase + 1][t0:t1, h + 1, EDGE : EDGE + W, :] = value * silu_slope(
                        stored[t0:t1, h]
                    )
                else:
                    out[t0:t1, h] = value
            if phase < 2:
                send(phase + 1, group)

    for phase in range(3):
        for group in range(2):
            for dh, dw in SIDES:
                @pl.when(present(dh, dw))
                def _():
                    copy_to(phase, group, dh, dw).wait_send()


def local(cotangent, stored_first, stored_second, w_first, w_second, w_third):
    F, R, W, C = cotangent.shape
    sizes = (lax.axis_size("ha"), lax.axis_size("wa"), F, R, W, C)
    ext = pltpu.VMEM((F, R + 2, W + 2 * EDGE, C), jnp.float32)
    wbuf = pltpu.VMEM(w_first.shape, jnp.float32)
    stored = pltpu.VMEM((F, R, W, C), jnp.float32)
    return pl.pallas_call(
        functools.partial(kernel, sizes),
        out_shape=jax.ShapeDtypeStruct(cotangent.shape, jnp.float32),
        in_specs=[pl.BlockSpec(memory_space=pltpu.HBM)] * 6,
        out_specs=pl.BlockSpec(memory_space=pltpu.VMEM),
        scratch_shapes=[
            ext, ext, ext,
            pltpu.VMEM((F, R + 2, W, 6 * LANES), jnp.bfloat16),
            wbuf, wbuf, wbuf,
            pltpu.VMEM((3, 3, 3, 6 * LANES, LANES), jnp.bfloat16),
            pltpu.VMEM((F, R // 2, W, 2 * LANES), jnp.float32),
            stored, stored,
            pltpu.SemaphoreType.DMA((6,)),
            pltpu.SemaphoreType.DMA((3, 2, 8)),
            pltpu.SemaphoreType.DMA((3, 2, 8)),
        ],
        compiler_params=pltpu.CompilerParams(
            collective_id=0, has_side_effects=True, vmem_limit_bytes=67043328
        ),
    )(cotangent, stored_first, stored_second, w_first, w_second, w_third)


def solution(mesh):
    split_spec = P("clip", "ha", "wa", None)
    return jax.shard_map(
        local,
        mesh=mesh,
        in_specs=(split_spec, split_spec, split_spec, P(), P(), P()),
        out_specs=split_spec,
        check_vma=False,
    )
```

```python
import functools

import jax
import jax.numpy as jnp
from jax import lax
from jax.experimental import pallas as pl
from jax.experimental.pallas import tpu as pltpu
from jax.sharding import PartitionSpec as P

LANES = 128
EDGE = 8
SIDES = tuple((dh, dw) for dh in (-1, 0, 1) for dw in (-1, 0, 1) if (dh, dw) != (0, 0))
COLS = ((0, -1), (0, 1))
ROWS = tuple(s for s in SIDES if s[0] != 0)


def silu_slope(value):
    sigma = 1.0 / (1.0 + jnp.exp(-value))
    return sigma * (1.0 + value * (1.0 - sigma))


def split(value):
    high = value.astype(jnp.bfloat16)
    low = (value - high.astype(jnp.float32)).astype(jnp.bfloat16)
    return high, low


def kernel(
    sizes, cot, first, second, w1, w2, w3, out,
    ext0, ext1, ext2, xs, wbuf0, wbuf1, wbuf2, whl, acc, sfirst, ssecond,
    local_sem, send_sem, recv_sem,
):
    nh, nw, F, R, W, C = sizes
    span = 3 * LANES
    exts = (ext0, ext1, ext2)
    wbufs = (wbuf0, wbuf1, wbuf2)
    ih, iw = lax.axis_index("ha"), lax.axis_index("wa")

    def present(dh, dw):
        ok = ih >= 0
        if dh:
            ok = ok & ((ih > 0) if dh < 0 else (ih < nh - 1))
        if dw:
            ok = ok & ((iw > 0) if dw < 0 else (iw < nw - 1))
        return ok

    def one(flag):
        return jnp.where(flag, jnp.int32(1), jnp.int32(0))

    loads = [
        pltpu.make_async_copy(cot, ext0.at[:, pl.ds(1, R), pl.ds(EDGE, W), :], local_sem.at[0]),
        pltpu.make_async_copy(w3, wbuf0, local_sem.at[1]),
        pltpu.make_async_copy(w2, wbuf1, local_sem.at[2]),
        pltpu.make_async_copy(w1, wbuf2, local_sem.at[3]),
        pltpu.make_async_copy(second, ssecond, local_sem.at[4]),
        pltpu.make_async_copy(first, sfirst, local_sem.at[5]),
    ]
    for load in loads:
        load.start()

    barrier = pltpu.get_barrier_semaphore()
    for dh, dw in SIDES:
        @pl.when(present(dh, dw))
        def _():
            pl.semaphore_signal(
                barrier, inc=1, device_id={"ha": ih + dh, "wa": iw + dw},
                device_id_type=pl.DeviceIdType.MESH,
            )
    tall = 1 + one(ih > 0) + one(ih < nh - 1)
    wide = 1 + one(iw > 0) + one(iw < nw - 1)
    pl.semaphore_wait(barrier, tall * wide - 1)

    groups = ((F // 2, F), (0, F // 2))

    def copy_to(phase, group, dh, dw):
        t0, t1 = groups[group]
        row, rows = {-1: (0, 1), 0: (0, R), 1: (R - 1, 1)}[dh]
        col, cols = {-1: (0, EDGE), 0: (0, W), 1: (W - EDGE, EDGE)}[dw]
        drow = {-1: R + 1, 0: 1, 1: 0}[dh]
        dcol = {-1: EDGE + W, 0: EDGE, 1: 0}[dw]
        ext, frames = exts[phase], pl.ds(t0, t1 - t0)
        if phase == 0:
            src = cot.at[frames, pl.ds(row, rows), pl.ds(col, cols), :]
        else:
            src = ext.at[frames, pl.ds(row + 1, rows), pl.ds(col + EDGE, cols), :]
        at = SIDES.index((dh, dw))
        return pltpu.make_async_remote_copy(
            src_ref=src,
            dst_ref=ext.at[frames, pl.ds(drow, rows), pl.ds(dcol, cols), :],
            send_sem=send_sem.at[phase, group, at],
            recv_sem=recv_sem.at[phase, group, at],
            device_id={"ha": ih + dh, "wa": iw + dw},
            device_id_type=pl.DeviceIdType.MESH,
        )

    def send(phase, group):
        for dh, dw in COLS + ROWS:
            @pl.when(present(dh, dw))
            def _():
                copy_to(phase, group, dh, dw).start()

    def receive(phase, group, sides):
        for dh, dw in sides:
            @pl.when(present(-dh, -dw))
            def _():
                copy_to(phase, group, dh, dw).wait_recv()

    send(0, 0)
    send(0, 1)

    xs[...] = jnp.zeros_like(xs)
    for dh, dw in SIDES:
        @pl.when(jnp.logical_not(present(dh, dw)))
        def _():
            row, rows = {-1: (0, 1), 0: (1, R), 1: (R + 1, 1)}[dh]
            col, cols = {-1: (0, EDGE), 0: (EDGE, W), 1: (EDGE + W, EDGE)}[dw]
            for ext in exts:
                ext[:, row : row + rows, col : col + cols, :] = jnp.zeros(
                    (F, rows, cols, C), jnp.float32
                )

    def prepare(phase):
        wbuf = wbufs[phase]

        @pl.loop(0, 3)
        def _(i):
            for j in range(3):
                for k in range(3):
                    turned = split(jnp.transpose(wbuf[i, j, k]))
                    for part in range(2):
                        at = part * span + k * LANES
                        whl[phase, i, j, at : at + C, 0:C] = turned[part]
                        whl[phase, i, j, at + C : at + LANES, :] = jnp.zeros(
                            (LANES - C, LANES), jnp.bfloat16
                        )

    def arrange(phase, group, rows):
        ext = exts[phase]

        @pl.loop(*groups[group])
        def _(f):
            for e in rows:
                for k in range(3):
                    start = EDGE + 1 - k
                    high, low = split(ext[f, e, start : start + W, :])
                    xs[f, e, :, k * LANES : k * LANES + C] = high
                    xs[f, e, :, span + k * LANES : span + k * LANES + C] = low

    pairs = R // 2

    def reach(group, i):
        t0, t1 = groups[group]
        return t0, min(t1, F - 2 + i)

    def lhs(group, i, q):
        t0, t1 = reach(group, i)
        parts = [xs[t0 + 2 - i : t1 + 2 - i, 2 * p + q][:, None] for p in range(pairs)]
        block = jnp.concatenate(parts, axis=1).reshape((t1 - t0) * pairs * W, 2 * span)
        return jnp.concatenate([block, block[:, :span]], axis=1)

    def rhs(phase, i, j):
        high, low = whl[phase, i, j, :span], whl[phase, i, j, span:]
        return jnp.concatenate([high, high, low], axis=0)

    def dot(a, b):
        return jnp.dot(a, b, preferred_element_type=jnp.float32)

    def weights(phase, i, j):
        if 0 <= j <= 2:
            return rhs(phase, i, j)
        return jnp.zeros((3 * span, LANES), jnp.bfloat16)

    def multiply(phase, group, offsets, fresh):
        for i in (2, 1, 0):
            t0, t1 = reach(group, i)
            if t1 <= t0:
                continue
            a = jnp.concatenate([lhs(group, i, q) for q in offsets], axis=1)
            b = jnp.concatenate(
                [
                    jnp.concatenate([weights(phase, i, 2 - q), weights(phase, i, 3 - q)], axis=1)
                    for q in offsets
                ],
                axis=0,
            )
            value = dot(a, b).reshape(t1 - t0, pairs, W, 2 * LANES)
            if fresh and i == 2:
                acc[t0:t1] = value
            else:
                acc[t0:t1] += value

    for phase in range(3):
        loads[phase + 1].wait()
        prepare(phase)
    loads[0].wait()
    for phase in range(3):
        for group in range(2):
            t0, t1 = groups[group]
            if phase and group == 0:
                receive(phase, group, SIDES)
                arrange(phase, group, range(R + 2))
                multiply(phase, group, (0, 1, 2, 3), True)
            else:
                receive(phase, group, COLS)
                arrange(phase, group, range(1, R + 1))
                multiply(phase, group, (1, 2), True)
                receive(phase, group, ROWS)
                arrange(phase, group, (0, R + 1))
                multiply(phase, group, (0, 3), False)
            if phase < 2 and group == 0:
                loads[4 + phase].wait()
            for h in range(R):
                at = h % 2 * LANES
                value = acc[t0:t1, h // 2, :, at : at + C]
                if phase < 2:
                    stored = (ssecond, sfirst)[phase]
                    exts[phase + 1][t0:t1, h + 1, EDGE : EDGE + W, :] = value * silu_slope(
                        stored[t0:t1, h]
                    )
                else:
                    out[t0:t1, h] = value
            if phase < 2:
                send(phase + 1, group)

    for phase in range(3):
        for group in range(2):
            for dh, dw in SIDES:
                @pl.when(present(dh, dw))
                def _():
                    copy_to(phase, group, dh, dw).wait_send()


def local(cotangent, stored_first, stored_second, w_first, w_second, w_third):
    F, R, W, C = cotangent.shape
    sizes = (lax.axis_size("ha"), lax.axis_size("wa"), F, R, W, C)
    ext = pltpu.VMEM((F, R + 2, W + 2 * EDGE, C), jnp.float32)
    wbuf = pltpu.VMEM(w_first.shape, jnp.float32)
    stored = pltpu.VMEM((F, R, W, C), jnp.float32)
    return pl.pallas_call(
        functools.partial(kernel, sizes),
        out_shape=jax.ShapeDtypeStruct(cotangent.shape, jnp.float32),
        in_specs=[pl.BlockSpec(memory_space=pltpu.HBM)] * 6,
        out_specs=pl.BlockSpec(memory_space=pltpu.VMEM),
        scratch_shapes=[
            ext, ext, ext,
            pltpu.VMEM((F, R + 2, W, 6 * LANES), jnp.bfloat16),
            wbuf, wbuf, wbuf,
            pltpu.VMEM((3, 3, 3, 6 * LANES, LANES), jnp.bfloat16),
            pltpu.VMEM((F, R // 2, W, 2 * LANES), jnp.float32),
            stored, stored,
            pltpu.SemaphoreType.DMA((6,)),
            pltpu.SemaphoreType.DMA((3, 2, 8)),
            pltpu.SemaphoreType.DMA((3, 2, 8)),
        ],
        compiler_params=pltpu.CompilerParams(
            collective_id=0, has_side_effects=True, vmem_limit_bytes=67043328
        ),
    )(cotangent, stored_first, stored_second, w_first, w_second, w_third)


def solution(mesh):
    split_spec = P("clip", "ha", "wa", None)
    return jax.shard_map(
        local,
        mesh=mesh,
        in_specs=(split_spec, split_spec, split_spec, P(), P(), P()),
        out_specs=split_spec,
        check_vma=False,
    )
```
